512 devices in a mesh: dp: 16 (over x, y_lo, core), pipe: 8 (over z), tensor: 4 (over y_hi).
Axes of the slice: x: 4, y: 8 (y_hi: 4, y_lo: 2; y = y_hi * 2 + y_lo), z: 8, core: 2. Of those that a mesh axis runs over, the one named last changes fastest.
Arguments:
- weights: bfloat16 [11264, 1408], P(('dp', 'pipe', 'tensor')), may hold values from -6 to 6
- first_moment: bfloat16 [11264, 1408], P(('dp', 'pipe', 'tensor')), may hold values from -6 to 6
- second_moment: bfloat16 [11264, 1408], P(('dp', 'pipe', 'tensor')), may hold values from 0.049804688 to 5
- row_weight: float32 [1408], replicated, may hold values from -1 to 1
- col_weight: float32 [1408], replicated, may hold values from 1 to 4
Outputs:
- weight_tiles: bfloat16 [11264, 1408], P(('pipe', 'tensor'))
- first_tiles: bfloat16 [11264, 1408], P(('pipe', 'tensor'))
- second_tiles: bfloat16 [11264, 1408], P(('pipe', 'tensor'))
- checksums: float32 [3, 8, 4, 11], P(None, 'pipe', 'tensor')
The draws below stay inside these ranges and needn't reach their ends.
All inputs are finite; a program needn't handle non-finite values.
Results may differ from the reference program's by a relative error of at most 0.001.
Values may be sent and summed in bfloat16 or wider, within the bound.
A program may use at most 64 MiB of HBM per device.

```python
import math
import jax
import jax.numpy as jnp
from jax import lax

D = 1408
CHECK_COLS = 128
BLOCKS = 8
N_TENSOR = 4


def block_scale(key, dims, shards, low, high):
    gain = 1.0
    for position, blocks in shards:
        heights = jax.random.uniform(jax.random.fold_in(jax.random.fold_in(key, 6), position), (blocks,), jnp.float32, low / len(shards), high / len(shards))
        gain = gain * jnp.repeat(jnp.exp(heights), dims[position] // blocks).reshape((-1,) + (1,) * (len(dims) - 1 - position))
    return gain


def scatter_about(stream_key, dims, width, bound, pieces=(), kind=jnp.bfloat16):
    values = width * jax.random.normal(stream_key, dims, jnp.float32)
    if pieces:
        values = values * block_scale(stream_key, dims, pieces, -0.22, 0.18)
    return jnp.clip(values, -bound, bound).astype(kind)


def setup_inputs(seed: int = 0) -> dict:
    seeds = jax.random.split(jax.random.key(seed), 6)
    return {
        "weights": scatter_about(seeds[0], (BLOCKS * D, D), 1.0, 6.0, ((0, 512),)),
        "first_moment": scatter_about(seeds[1], (BLOCKS * D, D), 1.0, 6.0, ((0, 512),)),
        "second_moment": jnp.clip(jnp.exp(math.log(5.0) - 4.609084 * jax.random.uniform(seeds[2], (BLOCKS * D, D), jnp.float32) ** block_scale(seeds[2], (BLOCKS * D, D), ((0, 512),), -0.2, 0.2)), 0.049804688, 5.0).astype(jnp.bfloat16),
        "row_weight": jnp.clip(jax.random.uniform(seeds[3], (D,), jnp.float32, -1.0, 1.0), -1.0, 1.0),
        "col_weight": jnp.clip(jnp.exp(jax.random.uniform(seeds[4], (D,), jnp.float32, math.log(1.0), math.log(4.0))), 1.0, 4.0),
    }


def reference(weights, first_moment, second_moment, row_weight, col_weight):
    tile_rows = D // N_TENSOR
    col_blocks = D // CHECK_COLS
    factor = float(tile_rows * CHECK_COLS) ** -0.5
    row_grid = row_weight.reshape(N_TENSOR, tile_rows)
    col_grid = col_weight.reshape(col_blocks, CHECK_COLS)

    def one_kind(data):
        blocked = data.astype(jnp.float32).reshape(BLOCKS, N_TENSOR, tile_rows, col_blocks, CHECK_COLS)
        weighted = jnp.einsum("bjrce,jr->bjce", blocked, row_grid, precision=lax.Precision.HIGHEST)
        return factor * jnp.sum(weighted * col_grid, axis=3)

    checks = jnp.stack([one_kind(weights), one_kind(first_moment), one_kind(second_moment)]).astype(jnp.float32)
    return weights, first_moment, second_moment, checks
```

```python
import jax
import jax.numpy as jnp
from jax import lax
from jax.experimental import pallas as pl
from jax.experimental.pallas import tpu as pltpu
from jax.sharding import PartitionSpec as P

MESH = pl.DeviceIdType.MESH
CHECK_COLS = 128
X_SLOT, Z_SLOT, OWN_SLOT, SLOTS = 16, 17, 19, 20


def kernel(
    w_ref, m_ref, v_ref, row_ref, col_ref, wo_ref, mo_ref, vo_ref, check_ref,
    held, row_part, in_sem, x_sem, z_sem, got_sem, send_sem,
):
    sources, tiles = (w_ref, m_ref, v_ref), (wo_ref, mo_ref, vo_ref)
    rows = w_ref.shape[0]
    width = w_ref.shape[1]
    tile_rows = wo_ref.shape[0]
    d, z, yh = lax.axis_index("dp"), lax.axis_index("pipe"), lax.axis_index("tensor")
    x, yl, c = d // 4, (d // 2) % 2, d % 2
    sign = 1 - 2 * c

    def at(x_, yl_, c_, z_=None, yh_=None):
        return {
            "dp": x_ * 4 + yl_ * 2 + c_,
            "pipe": z if z_ is None else z_,
            "tensor": yh if yh_ is None else yh_,
        }

    sends = []

    def send(src, dst, sem, to, condition=None):
        copy = pltpu.make_async_remote_copy(
            src_ref=src,
            dst_ref=dst,
            send_sem=send_sem.at[len(sends)],
            recv_sem=sem,
            device_id=to,
            device_id_type=MESH,
        )
        sends.append((condition, copy))
        if condition is None:
            copy.start()
        else:
            pl.when(condition)(copy.start)

    core_mate = at(x, yl, 1 - c)

    def arrive(ref, sem):
        pltpu.make_async_remote_copy(
            src_ref=ref, dst_ref=ref, send_sem=send_sem.at[0], recv_sem=sem,
            device_id=core_mate, device_id_type=MESH,
        ).wait_recv()

    x_to = (z + 8 - x - yl) % 4
    x_moves = x_to != x
    x_mate = at(x_to, yl, c)
    z_to = 2 * x_to + yl
    z_moves = z_to != z
    z_dest = at(x, yl, c, z_=z_to)
    even = z % 2 == yl
    quarter = (z // 2 + z % 2 + x) % 4
    y_place = 4 * quarter + yh
    y_dests = [at(x, yh % 2, yh // 2, yh_=2 * c + h) for h in range(2)]
    own = 4 * quarter + yl + 2 * c
    y_source = at(x, z % 2, yh // 2, yh_=yl + 2 * c)
    stays = jnp.logical_and(even, jnp.logical_and(yh == yl + 2 * c, c == yh // 2))

    barrier = pltpu.get_barrier_semaphore()
    y_mate = at(x, 1 - yl, c)
    x_next = {s: at((x + 4 + s * sign) % 4, yl, c) for s in (1, -1)}

    def greet(to):
        pl.semaphore_signal(barrier, inc=1, device_id=to, device_id_type=MESH)

    for to in (x_mate, y_source, y_mate, x_next[1], x_next[-1], core_mate):
        greet(to)

    @pl.when(even)
    def _():
        greet(at(x, yl, c, z_=quarter))
        greet(at(x, yl, c, z_=quarter + 4))

    loads = []
    for a in range(3):
        load = pltpu.make_async_copy(sources[a], held.at[a, OWN_SLOT], in_sem.at[a])
        load.start()
        loads.append(load)

    for j in range(tile_rows // rows // 4):

        @pl.when(yh == j)
        def _():
            row_part[...] = row_ref[:, j * tile_rows : (j + 1) * tile_rows]

    pl.semaphore_wait(barrier, 6 + 2 * even.astype(jnp.int32))

    for a in range(3):
        loads[a].wait()
        send(held.at[a, OWN_SLOT], held.at[a, X_SLOT], x_sem.at[a], x_mate, x_moves)
    x_slot = jnp.where(x_moves, X_SLOT, OWN_SLOT)
    half = z // 4
    for a in range(3):

        @pl.when(x_moves)
        def _():
            arrive(held.at[a, X_SLOT], x_sem.at[a])

        send(held.at[a, x_slot], held.at[a, Z_SLOT + half], z_sem.at[half, a], z_dest, z_moves)
    here = [jnp.logical_and(even, quarter + 4 * h == z) for h in range(2)]
    away = [jnp.logical_and(even, quarter + 4 * h != z) for h in range(2)]
    z_slot = [jnp.where(here[h], x_slot, Z_SLOT + h) for h in range(2)]
    for a in range(3):
        for h in range(2):

            @pl.when(away[h])
            def _():
                arrive(held.at[a, Z_SLOT + h], z_sem.at[h, a])

            mine = jnp.logical_and(stays, yh % 2 == h)
            send(
                held.at[a, z_slot[h]], held.at[a, y_place], got_sem.at[a, y_place], y_dests[h],
                jnp.logical_and(even, jnp.logical_not(mine)),
            )
    own_slot = jnp.where(stays, jnp.where(yh % 2 == 0, z_slot[0], z_slot[1]), own)

    def slot(dx, other):
        row = 1 - yl if other else yl
        return 4 * ((z // 2 + z % 2 + x + 4 + dx * sign) % 4) + row + 2 * c

    def pass_on(a, dx, other, to, wait=True):
        k = slot(dx, other)
        src = k
        if dx == 0 and not other:
            src = own_slot

            @pl.when(jnp.logical_not(stays))
            def _():
                arrive(held.at[a, k], got_sem.at[a, k])

        else:
            arrive(held.at[a, k], got_sem.at[a, k])
        for dest in to:
            send(held.at[a, src], held.at[a, k], got_sem.at[a, k], dest)

    xs = (x_next[1], x_next[-1])
    pass_on(0, 0, 0, (*xs, y_mate, core_mate))
    pass_on(1, 0, 0, (y_mate, *xs, core_mate))
    pass_on(2, 0, 0, (y_mate, *xs, core_mate))
    pass_on(0, -1, 0, (x_next[1], y_mate, core_mate))
    pass_on(1, 0, 1, (*xs, core_mate))
    pass_on(2, 0, 1, (*xs, core_mate))
    pass_on(0, 1, 0, (y_mate, core_mate))
    for a in (1, 2):
        pass_on(a, -1, 0, (x_next[1], core_mate))
    for a in (1, 2):
        pass_on(a, -1, 1, (x_next[1], core_mate))
    pass_on(0, 2, 0, (y_mate, core_mate))
    for dx in (0, -1, 1):
        pass_on(0, dx, 1, (core_mate,))
    for other in (0, 1):
        for a in (1, 2):
            pass_on(a, 1, other, (core_mate,))
    for other in (0, 1):
        for a in (1, 2):
            pass_on(a, 2, other, (core_mate,))
    pass_on(0, 2, 1, (core_mate,))

    for a in range(3):

        @pl.when(stays)
        def _():
            held[a, own] = held[a, own_slot]

    part = row_part[...]
    high = part.astype(jnp.bfloat16).astype(jnp.float32)
    middle = (part - high).astype(jnp.bfloat16).astype(jnp.float32)
    low = part - high - middle
    line = lax.broadcasted_iota(jnp.int32, (8, tile_rows), 0)
    left = jnp.where(line == 0, high, jnp.where(line == 1, middle, jnp.where(line == 2, low, 0.0)))
    left = left.astype(jnp.bfloat16)
    factor = float(tile_rows * CHECK_COLS) ** (-0.5)
    weight = col_ref[...] * factor
    lane = lax.broadcasted_iota(jnp.int32, (1, CHECK_COLS), 1)
    for a in range(3):
        for k in range(16):

            @pl.when(c != (k % 4) // 2)
            def _():
                arrive(held.at[a, k], got_sem.at[a, k])

            tiles[a][k * rows : (k + 1) * rows, :] = held[a, k]
        mixed = jnp.dot(left, tiles[a][...], preferred_element_type=jnp.float32)
        mixed = jnp.sum(mixed, axis=0, keepdims=True) * weight
        sums = jnp.zeros((1, CHECK_COLS), jnp.float32)
        for e in range(width // CHECK_COLS):
            piece = mixed[:, e * CHECK_COLS : (e + 1) * CHECK_COLS]
            sums = jnp.where(lane == e, jnp.sum(piece, axis=1, keepdims=True), sums)
        check_ref[a, 0] = sums[:, : width // CHECK_COLS]

    for condition, copy in sends:
        if condition is None:
            copy.wait_send()
        else:
            pl.when(condition)(copy.wait_send)


def shards(weights, first_moment, second_moment, row_weight, col_weight):
    rows, width = weights.shape
    tile_rows = rows * 16
    whole = pl.BlockSpec(memory_space=pltpu.VMEM)
    tile = jax.ShapeDtypeStruct((tile_rows, width), jnp.bfloat16)
    return pl.pallas_call(
        kernel,
        out_shape=(
            tile, tile, tile,
            jax.ShapeDtypeStruct((3, 1, 1, width // CHECK_COLS), jnp.float32),
        ),
        in_specs=[pl.BlockSpec(memory_space=pl.ANY)] * 3 + [whole] * 2,
        out_specs=(whole,) * 4,
        scratch_shapes=[
            pltpu.VMEM((3, SLOTS, rows, width), jnp.bfloat16),
            pltpu.VMEM((1, tile_rows), jnp.float32),
            pltpu.SemaphoreType.DMA((3,)),
            pltpu.SemaphoreType.DMA((3,)),
            pltpu.SemaphoreType.DMA((2, 3)),
            pltpu.SemaphoreType.DMA((3, 16)),
            pltpu.SemaphoreType.DMA((64,)),
        ],
        compiler_params=pltpu.CompilerParams(collective_id=0, has_side_effects=True),
    )(
        weights, first_moment, second_moment,
        row_weight.reshape(1, width), col_weight.reshape(1, width),
    )


def solution(mesh):
    flat = P(("dp", "pipe", "tensor"), None)
    tile = P(("pipe", "tensor"), None)
    return jax.shard_map(
        shards,
        mesh=mesh,
        in_specs=(flat, flat, flat, P(), P()),
        out_specs=(tile, tile, tile, P(None, "pipe", "tensor", None)),
        check_vma=False,
    )
```

```python
import jax
import jax.numpy as jnp
from jax import lax
from jax.experimental import pallas as pl
from jax.experimental.pallas import tpu as pltpu
from jax.sharding import PartitionSpec as P

MESH = pl.DeviceIdType.MESH
CHECK_COLS = 128
X_SLOT, Z_SLOT, OWN_SLOT, SLOTS = 16, 17, 19, 20


def chunks_of(width):
    return [(a, slice(0, width)) for a in range(3)]


def kernel(
    w_ref, m_ref, v_ref, row_ref, col_ref, wo_ref, mo_ref, vo_ref, check_ref,
    held, row_all, col_all, row_part, in_sem, x_sem, z_sem, got_sem, send_sem,
):
    sources, tiles = (w_ref, m_ref, v_ref), (wo_ref, mo_ref, vo_ref)
    rows, width = w_ref.shape
    tile_rows = wo_ref.shape[0]
    chunks = chunks_of(width)
    d, z, yh = lax.axis_index("dp"), lax.axis_index("pipe"), lax.axis_index("tensor")
    x, yl, c = d // 4, (d // 2) % 2, d % 2
    sign = 1 - 2 * c

    def at(x_, yl_, c_, z_=None, yh_=None):
        return {
            "dp": x_ * 4 + yl_ * 2 + c_,
            "pipe": z if z_ is None else z_,
            "tensor": yh if yh_ is None else yh_,
        }

    core_mate, y_mate = at(x, yl, 1 - c), at(x, 1 - yl, c)
    x_next = {s: at((x + 4 + s * sign) % 4, yl, c) for s in (1, -1)}
    sends = []

    def piece(i, slot):
        a, columns = chunks[i]
        return held.at[a, slot, :, columns]

    def send(i, src, dst, sem, to, condition=None):
        copy = pltpu.make_async_remote_copy(
            src_ref=piece(i, src),
            dst_ref=piece(i, dst),
            send_sem=send_sem.at[len(sends)],
            recv_sem=sem,
            device_id=to,
            device_id_type=MESH,
        )
        sends.append((condition, copy))
        if condition is None:
            copy.start()
        else:
            pl.when(condition)(copy.start)

    def arrive(i, slot, sem, condition=None):
        copy = pltpu.make_async_remote_copy(
            src_ref=piece(i, slot), dst_ref=piece(i, slot), send_sem=send_sem.at[0],
            recv_sem=sem, device_id=core_mate, device_id_type=MESH,
        )
        if condition is None:
            copy.wait_recv()
        else:
            pl.when(condition)(copy.wait_recv)

    x_to = (z + 8 - x - yl) % 4
    x_moves = x_to != x
    x_mate = at(x_to, yl, c)
    z_to = 2 * x_to + yl
    z_moves = z_to != z
    z_dest = at(x, yl, c, z_=z_to)
    half = z // 4
    even = z % 2 == yl
    quarter = (z // 2 + z % 2 + x) % 4
    y_place = 4 * quarter + yh
    special = yh % 2
    own_half = c == yh // 2

    def y_dest(h, row):
        return at(x, row, yh // 2, yh_=2 * c + h)

    own = [4 * quarter + 2 * c + u for u in range(2)]
    y_source = [at(x, z % 2, yh // 2, yh_=2 * c + u) for u in range(2)]
    stays = [jnp.logical_and(even, jnp.logical_and(special == u, own_half)) for u in range(2)]
    handed = [
        jnp.logical_and(even, jnp.logical_and(special == u, jnp.logical_not(own_half))) for u in range(2)
    ]
    hands_on = [
        jnp.logical_and(
            jnp.logical_not(even), jnp.logical_and(special == u, jnp.logical_not(own_half))
        )
        for u in range(2)
    ]

    barrier = pltpu.get_barrier_semaphore()

    def greet(to):
        pl.semaphore_signal(barrier, inc=1, device_id=to, device_id_type=MESH)

    @pl.when(even)
    def _():
        greet(at(x, yl, c, z_=quarter))
        greet(at(x, yl, c, z_=quarter + 4))

    for to in (x_mate, x_next[1], x_next[-1], core_mate):
        greet(to)
    for u in range(2):
        direct = jnp.logical_not(jnp.logical_and(even, special == u))
        pl.when(direct)(lambda u=u: greet(y_source[u]))
        pl.when(handed[u])(lambda: greet(y_mate))

    loads = []
    for i in range(len(chunks)):
        a, columns = chunks[i]
        load = pltpu.make_async_copy(sources[a].at[:, columns], piece(i, OWN_SLOT), in_sem.at[i])
        load.start()
        loads.append(load)

    weight_loads = [
        pltpu.make_async_copy(row_ref, row_all, in_sem.at[len(chunks)]),
        pltpu.make_async_copy(col_ref, col_all, in_sem.at[len(chunks) + 1]),
    ]
    for load in weight_loads:
        load.start()

    count = 5 + 3 * even.astype(jnp.int32) + jnp.logical_or(hands_on[0], hands_on[1]).astype(jnp.int32)
    pl.semaphore_wait(barrier, count)

    each = range(len(chunks))
    for i in each:
        loads[i].wait()
        send(i, OWN_SLOT, X_SLOT, x_sem.at[i], x_mate, x_moves)
    x_slot = jnp.where(x_moves, X_SLOT, OWN_SLOT)
    for i in each:
        arrive(i, X_SLOT, x_sem.at[i], x_moves)
        send(i, x_slot, Z_SLOT + half, z_sem.at[half, i], z_dest, z_moves)
    away = [jnp.logical_and(even, quarter + 4 * h != z) for h in range(2)]
    z_slot = [jnp.where(quarter + 4 * h == z, x_slot, Z_SLOT + h) for h in range(2)]
    for i in each:
        for h in range(2):
            arrive(i, Z_SLOT + h, z_sem.at[h, i], away[h])
            got = got_sem.at[i, y_place]
            send(i, z_slot[h], y_place, got, y_dest(h, 1 - yl), even)
            normal = jnp.logical_and(even, special != h)
            send(i, z_slot[h], y_place, got, y_dest(h, yl), normal)
    own_slot = [jnp.where(stays[u], z_slot[u], own[u]) for u in range(2)]

    def mine(i):
        for u in range(2):
            got = got_sem.at[i, own[u]]
            arrive(i, own[u], got, jnp.logical_not(stays[u]))
            for to in (x_next[1], x_next[-1]):
                send(i, own_slot[u], own[u], got, to)
            send(i, own[u], own[u], got, y_mate, hands_on[u])
            send(i, own_slot[u], own[u], got, core_mate)

    def theirs(i, dx):
        for u in range(2):
            k = 4 * ((quarter + 4 + dx * sign) % 4) + 2 * c + u
            got = got_sem.at[i, k]
            arrive(i, k, got)
            if dx == -1:
                send(i, k, k, got, x_next[1])
            send(i, k, k, got, core_mate)

    for i in range(len(chunks) + 2):
        if i < len(chunks):
            mine(i)
        if 0 <= i - 1 < len(chunks):
            theirs(i - 1, -1)
            theirs(i - 1, 1)
        if 0 <= i - 2 < len(chunks):
            theirs(i - 2, 2)

    for u in range(2):

        @pl.when(stays[u])
        def _():
            for a in range(3):
                held[a, own[u]] = held[a, own_slot[u]]

    for load in weight_loads:
        load.wait()
    for j in range(width // tile_rows):

        @pl.when(yh == j)
        def _():
            row_part[0] = row_all[pl.ds(j * tile_rows, tile_rows)]
    part = row_part[...]
    high = part.astype(jnp.bfloat16).astype(jnp.float32)
    middle = (part - high).astype(jnp.bfloat16).astype(jnp.float32)
    low = part - high - middle
    line = lax.broadcasted_iota(jnp.int32, (8, tile_rows), 0)
    left = jnp.where(line == 0, high, jnp.where(line == 1, middle, jnp.where(line == 2, low, 0.0)))
    left = left.astype(jnp.bfloat16)
    factor = float(tile_rows * CHECK_COLS) ** (-0.5)
    weight = col_all[...].reshape(1, width) * factor
    lane = lax.broadcasted_iota(jnp.int32, (1, CHECK_COLS), 1)
    for a in range(3):
        for k in range(16):
            for i in each:
                if chunks[i][0] == a:
                    arrive(i, k, got_sem.at[i, k], c != (k % 4) // 2)
            tiles[a][k * rows : (k + 1) * rows, :] = held[a, k]
        mixed = jnp.dot(left, tiles[a][...], preferred_element_type=jnp.float32)
        mixed = jnp.sum(mixed, axis=0, keepdims=True) * weight
        sums = jnp.zeros((1, CHECK_COLS), jnp.float32)
        for e in range(width // CHECK_COLS):
            part_sum = jnp.sum(mixed[:, e * CHECK_COLS : (e + 1) * CHECK_COLS], axis=1, keepdims=True)
            sums = jnp.where(lane == e, part_sum, sums)
        check_ref[a, 0] = sums[:, : width // CHECK_COLS]

    for condition, copy in sends:
        if condition is None:
            copy.wait_send()
        else:
            pl.when(condition)(copy.wait_send)


def store(*refs):
    n = len(refs) // 2
    ins, outs, sem = refs[:n], refs[n : 2 * n], refs[2 * n]
    copies = [pltpu.make_async_copy(ins[i], outs[i], sem.at[i]) for i in range(n)]
    for copy in copies:
        copy.start()
    for copy in copies:
        copy.wait()


def shards(weights, first_moment, second_moment, row_weight, col_weight):
    rows, width = weights.shape
    tile_rows = rows * 16
    n = len(chunks_of(width))
    whole = pl.BlockSpec(memory_space=pltpu.VMEM)
    tile = ((tile_rows, width), jnp.bfloat16)
    check = ((3, 1, 1, width // CHECK_COLS), jnp.float32)
    made = pl.pallas_call(
        kernel,
        out_shape=(pltpu.VMEM(*tile),) * 3 + (pltpu.VMEM(*check),),
        in_specs=[pl.BlockSpec(memory_space=pltpu.HBM)] * 5,
        out_specs=(whole,) * 4,
        scratch_shapes=[
            pltpu.VMEM((3, SLOTS, rows, width), jnp.bfloat16),
            pltpu.VMEM((width,), jnp.float32),
            pltpu.VMEM((width,), jnp.float32),
            pltpu.VMEM((1, tile_rows), jnp.float32),
            pltpu.SemaphoreType.DMA((n + 2,)),
            pltpu.SemaphoreType.DMA((n,)),
            pltpu.SemaphoreType.DMA((2, n)),
            pltpu.SemaphoreType.DMA((n, 16)),
            pltpu.SemaphoreType.DMA((n * 24,)),
        ],
        compiler_params=pltpu.CompilerParams(
            collective_id=0, has_side_effects=True, vmem_limit_bytes=60 * 2**20
        ),
    )(weights, first_moment, second_moment, row_weight, col_weight)
    return pl.pallas_call(
        store,
        out_shape=(jax.ShapeDtypeStruct(*tile),) * 3 + (jax.ShapeDtypeStruct(*check),),
        in_specs=[whole] * 4,
        out_specs=(pl.BlockSpec(memory_space=pltpu.HBM),) * 4,
        scratch_shapes=[pltpu.SemaphoreType.DMA((4,))],
        compiler_params=pltpu.CompilerParams(vmem_limit_bytes=2**20),
    )(*made)


def solution(mesh):
    flat = P(("dp", "pipe", "tensor"), None)
    tile = P(("pipe", "tensor"), None)
    return jax.shard_map(
        shards,
        mesh=mesh,
        in_specs=(flat, flat, flat, P(), P()),
        out_specs=(tile, tile, tile, P(None, "pipe", "tensor", None)),
        check_vma=False,
    )
```

```python
import jax
import jax.numpy as jnp
from jax import lax
from jax.experimental import pallas as pl
from jax.experimental.pallas import tpu as pltpu
from jax.sharding import PartitionSpec as P

MESH = pl.DeviceIdType.MESH
CHECK_COLS = 128
X_SLOT, Z_SLOT, OWN_SLOT, SLOTS = 16, 17, 19, 20
ONE_ROW = (0,)


def chunks_of(width):
    return [(a, slice(0, width)) for a in range(3)]


def kernel(
    w_ref, m_ref, v_ref, row_ref, col_ref, wo_ref, mo_ref, vo_ref, check_ref,
    held, row_all, col_all, row_part, in_sem, x_sem, z_sem, got_sem, send_sem, z_ready,
):
    sources, tiles = (w_ref, m_ref, v_ref), (wo_ref, mo_ref, vo_ref)
    rows, width = w_ref.shape
    tile_rows = wo_ref.shape[0]
    chunks = chunks_of(width)
    d, z, yh = lax.axis_index("dp"), lax.axis_index("pipe"), lax.axis_index("tensor")
    x, yl, c = d // 4, (d // 2) % 2, d % 2
    sign = 1 - 2 * c

    def at(x_, yl_, c_, z_=None, yh_=None):
        return {
            "dp": x_ * 4 + yl_ * 2 + c_,
            "pipe": z if z_ is None else z_,
            "tensor": yh if yh_ is None else yh_,
        }

    core_mate, y_mate = at(x, yl, 1 - c), at(x, 1 - yl, c)
    x_next = {s: at((x + 4 + s * sign) % 4, yl, c) for s in (1, -1)}
    sends = []

    def piece(i, slot):
        a, columns = chunks[i]
        return held.at[a, slot, :, columns]

    def send(i, src, dst, sem, to, condition=None):
        copy = pltpu.make_async_remote_copy(
            src_ref=piece(i, src),
            dst_ref=piece(i, dst),
            send_sem=send_sem.at[len(sends)],
            recv_sem=sem,
            device_id=to,
            device_id_type=MESH,
        )
        sends.append((condition, copy))
        if condition is None:
            copy.start()
        else:
            pl.when(condition)(copy.start)

    def arrive(i, slot, sem, condition=None):
        copy = pltpu.make_async_remote_copy(
            src_ref=piece(i, slot), dst_ref=piece(i, slot), send_sem=send_sem.at[0],
            recv_sem=sem, device_id=core_mate, device_id_type=MESH,
        )
        if condition is None:
            copy.wait_recv()
        else:
            pl.when(condition)(copy.wait_recv)

    x_to = (z + 8 - x - yl + 2 * c) % 4
    x_moves = x_to != x
    x_mate = at(x_to, yl, c)
    z_to = 2 * x_to + yl
    z_dest = at(x, yl, c, z_=z_to)
    half = z // 4
    even = z % 2 == yl
    came = (z // 2 + z % 2 + x + 2 * c) % 4
    quarter = (z // 2 + z % 2 + x + 2 * (yh // 2)) % 4
    y_place = 4 * came + yh
    special = yh % 2
    own_half = c == yh // 2

    def y_dest(h, row):
        return at(x, row, yh // 2, yh_=2 * c + h)

    order = (1 - special, special)
    own = [4 * quarter + 2 * c + u for u in order]
    y_source = [at(x, z % 2, yh // 2, yh_=2 * c + u) for u in order]
    stays = jnp.logical_and(even, own_half)
    handed = jnp.logical_and(even, jnp.logical_not(own_half))
    hands_on = jnp.logical_not(jnp.logical_or(even, own_half))
    one_stays = jnp.logical_and(stays, special == yl)
    one_far = jnp.logical_and(handed, special == yl)

    barrier = pltpu.get_barrier_semaphore()

    def greet(to):
        pl.semaphore_signal(barrier, inc=1, device_id=to, device_id_type=MESH)

    for h in range(2):
        z_from = came + 4 * h
        pl.when(jnp.logical_and(even, z_from > z))(lambda z_from=z_from: greet(at(x, yl, c, z_=z_from)))
    pl.when(z_to > z)(lambda: greet(z_dest))
    for to in (x_mate, x_next[1], x_next[-1], core_mate):
        greet(to)
    greet(y_source[0])
    pl.when(jnp.logical_not(even))(lambda: greet(y_source[1]))
    greet(y_mate)
    pl.when(one_far)(lambda: greet(y_source[1]))

    loads = []
    for i in range(len(chunks)):
        a, columns = chunks[i]
        load = pltpu.make_async_copy(sources[a].at[:, columns], piece(i, OWN_SLOT), in_sem.at[i])
        load.start()
        loads.append(load)

    weight_loads = [
        pltpu.make_async_copy(row_ref, row_all, in_sem.at[len(chunks)]),
        pltpu.make_async_copy(col_ref, col_all, in_sem.at[len(chunks) + 1]),
    ]
    for load in weight_loads:
        load.start()

    count = 5 + 3 * even.astype(jnp.int32) + one_far.astype(jnp.int32)
    count = count + (z_to < z).astype(jnp.int32)
    for h in range(2):
        count = count + jnp.logical_and(even, came + 4 * h < z).astype(jnp.int32)
    pl.semaphore_wait(barrier, count)
    for h in range(2):
        z_from = came + 4 * h

        @pl.when(jnp.logical_and(even, z_from < z))
        def _():
            pl.semaphore_signal(
                z_ready, inc=1, device_id=at(x, yl, c, z_=z_from), device_id_type=MESH
            )

    each = range(len(chunks))
    for i in each:
        loads[i].wait()
        send(i, OWN_SLOT, X_SLOT, x_sem.at[i], x_mate, x_moves)
    x_slot = jnp.where(x_moves, X_SLOT, OWN_SLOT)
    def z_send(i, condition):
        send(i, x_slot, Z_SLOT + half, z_sem.at[half, i], z_dest, condition)

    for i in each:
        arrive(i, X_SLOT, x_sem.at[i], x_moves)
        if i == 0:
            pl.when(z_to > z)(lambda: pl.semaphore_wait(z_ready, 1))
        z_send(i, z_to != z)
    away = [jnp.logical_and(even, came + 4 * h != z) for h in range(2)]
    z_slot = [jnp.where(came + 4 * h == z, x_slot, Z_SLOT + h) for h in range(2)]
    for h, i in [(h, i) for h in range(2) for i in each]:
        arrive(i, Z_SLOT + h, z_sem.at[h, i], away[h])
        got = got_sem.at[i, y_place]
        if chunks[i][0] in ONE_ROW:
            goes = jnp.logical_and(even, jnp.logical_not(jnp.logical_and(one_stays, special == h)))
            send(i, z_slot[h], y_place, got, y_dest(h, special), goes)
        else:
            send(i, z_slot[h], y_place, got, y_dest(h, 1 - yl), even)
            normal = jnp.logical_and(even, special != h)
            send(i, z_slot[h], y_place, got, y_dest(h, yl), normal)
    stay_slot = jnp.where(special == 0, z_slot[0], z_slot[1])
    own_slot = [own[0], jnp.where(stays, stay_slot, own[1])]
    one = 4 * quarter + yl + 2 * c
    one_slot = jnp.where(one_stays, stay_slot, one)

    def one_mine(i):
        got = got_sem.at[i, one]
        arrive(i, one, got, jnp.logical_not(one_stays))
        for to in (x_next[1], x_next[-1], y_mate, core_mate):
            send(i, one_slot, one, got, to)

    def one_theirs(i, dx, row):
        k = 4 * ((quarter + 4 + dx * sign) % 4) + 2 * c + (1 - yl if row else yl)
        got = got_sem.at[i, k]
        arrive(i, k, got)
        if row == 0:
            if dx == -1:
                send(i, k, k, got, x_next[1])
            send(i, k, k, got, y_mate)
        send(i, k, k, got, core_mate)

    def mine(i):
        if chunks[i][0] in ONE_ROW:
            return one_mine(i)
        for u in range(2):
            got = got_sem.at[i, own[u]]
            arrive(i, own[u], got, None if u == 0 else jnp.logical_not(stays))
            for to in (x_next[1], x_next[-1]):
                send(i, own_slot[u], own[u], got, to)
            if u == 1:
                send(i, own[u], own[u], got, y_mate, hands_on)
            send(i, own_slot[u], own[u], got, core_mate)

    def theirs(i, dx):
        if chunks[i][0] in ONE_ROW:
            return one_theirs(i, dx, 0)
        for u in range(2):
            k = 4 * ((quarter + 4 + dx * sign) % 4) + 2 * c + order[u]
            got = got_sem.at[i, k]
            arrive(i, k, got)
            if dx == -1:
                send(i, k, k, got, x_next[1])
            send(i, k, k, got, core_mate)

    def tile_of(a):
        place, source, stayed = (one, one_slot, one_stays) if a in ONE_ROW else (own[1], own_slot[1], stays)

        @pl.when(stayed)
        def _():
            held[a, place] = held[a, source]

        if a == 0:
            for load in weight_loads:
                load.wait()
            for j in range(width // tile_rows):

                @pl.when(yh == j)
                def _():
                    row_part[0] = row_all[pl.ds(j * tile_rows, tile_rows)]

        part = row_part[...]
        high = part.astype(jnp.bfloat16).astype(jnp.float32)
        middle = (part - high).astype(jnp.bfloat16).astype(jnp.float32)
        low = part - high - middle
        line = lax.broadcasted_iota(jnp.int32, (8, tile_rows), 0)
        left = jnp.where(line == 1, middle, jnp.where(line == 2, low, 0.0))
        left = jnp.where(line == 0, high, left).astype(jnp.bfloat16)
        factor = float(tile_rows * CHECK_COLS) ** (-0.5)
        weight = col_all[...].reshape(1, width) * factor
        lane = lax.broadcasted_iota(jnp.int32, (1, CHECK_COLS), 1)
        for k in range(16):
            for i in each:
                if chunks[i][0] == a:
                    arrive(i, k, got_sem.at[i, k], c != (k % 4) // 2)
            tiles[a][k * rows : (k + 1) * rows, :] = held[a, k]
        mixed = jnp.dot(left, tiles[a][...], preferred_element_type=jnp.float32)
        mixed = jnp.sum(mixed, axis=0, keepdims=True) * weight
        sums = jnp.zeros((1, CHECK_COLS), jnp.float32)
        for e in range(width // CHECK_COLS):
            part_sum = jnp.sum(mixed[:, e * CHECK_COLS : (e + 1) * CHECK_COLS], axis=1, keepdims=True)
            sums = jnp.where(lane == e, part_sum, sums)
        check_ref[a, 0] = sums[:, : width // CHECK_COLS]

    last = len(chunks)
    for i in range(last + 2):
        if i < last:
            mine(i)
        if 0 <= i - 1 < last:
            theirs(i - 1, -1)
            theirs(i - 1, 1)
        if 0 <= i - 2 < last:
            theirs(i - 2, 2)
        if 0 <= i - 3 < last and chunks[i - 3][0] in ONE_ROW:
            for dx in (0, -1, 1, 2):
                one_theirs(i - 3, dx, 1)
    for a in range(3):
        tile_of(a)

    for condition, copy in sends:
        if condition is None:
            copy.wait_send()
        else:
            pl.when(condition)(copy.wait_send)


def store(*refs):
    n = len(refs) // 2
    ins, outs, sem = refs[:n], refs[n : 2 * n], refs[2 * n]
    copies = [pltpu.make_async_copy(ins[i], outs[i], sem.at[i]) for i in range(n)]
    for copy in copies:
        copy.start()
    for copy in copies:
        copy.wait()


def shards(weights, first_moment, second_moment, row_weight, col_weight):
    rows, width = weights.shape
    tile_rows = rows * 16
    n = len(chunks_of(width))
    whole = pl.BlockSpec(memory_space=pltpu.VMEM)
    tile = ((tile_rows, width), jnp.bfloat16)
    check = ((3, 1, 1, width // CHECK_COLS), jnp.float32)
    made = pl.pallas_call(
        kernel,
        out_shape=(pltpu.VMEM(*tile),) * 3 + (pltpu.VMEM(*check),),
        in_specs=[pl.BlockSpec(memory_space=pltpu.HBM)] * 5,
        out_specs=(whole,) * 4,
        scratch_shapes=[
            pltpu.VMEM((3, SLOTS, rows, width), jnp.bfloat16),
            pltpu.VMEM((width,), jnp.float32),
            pltpu.VMEM((width,), jnp.float32),
            pltpu.VMEM((1, tile_rows), jnp.float32),
            pltpu.SemaphoreType.DMA((n + 2,)),
            pltpu.SemaphoreType.DMA((n,)),
            pltpu.SemaphoreType.DMA((2, n)),
            pltpu.SemaphoreType.DMA((n, 16)),
            pltpu.SemaphoreType.DMA((n * 24,)),
            pltpu.SemaphoreType.REGULAR,
        ],
        compiler_params=pltpu.CompilerParams(
            collective_id=0, has_side_effects=True, vmem_limit_bytes=60 * 2**20
        ),
    )(weights, first_moment, second_moment, row_weight, col_weight)
    return pl.pallas_call(
        store,
        out_shape=(jax.ShapeDtypeStruct(*tile),) * 3 + (jax.ShapeDtypeStruct(*check),),
        in_specs=[whole] * 4,
        out_specs=(pl.BlockSpec(memory_space=pltpu.HBM),) * 4,
        scratch_shapes=[pltpu.SemaphoreType.DMA((4,))],
        compiler_params=pltpu.CompilerParams(vmem_limit_bytes=2**20),
    )(*made)


def solution(mesh):
    flat = P(("dp", "pipe", "tensor"), None)
    tile = P(("pipe", "tensor"), None)
    return jax.shard_map(
        shards,
        mesh=mesh,
        in_specs=(flat, flat, flat, P(), P()),
        out_specs=(tile, tile, tile, P(None, "pipe", "tensor", None)),
        check_vma=False,
    )
```
